512 devices in a mesh: ia: 16 (over y_hi, z), ja: 8 (over y_lo, core), ka: 4 (over x).
Axes of the slice: x: 4, y: 8 (y_hi: 2, y_lo: 4; y = y_hi * 4 + y_lo), z: 8, core: 2. Of those that a mesh axis runs over, the one named last changes fastest.
Arguments:
- tile_values: bfloat16 [49152, 128], P(('ia', 'ja', 'ka')), may hold values from -0.59765625 to 0.59765625
- tile_rows: int32 [49152, 128], P(('ia', 'ja', 'ka')), may hold values from 0 to 63
- tile_cols: int32 [49152, 128], P(('ia', 'ja', 'ka')), may hold values from 0 to 8191
- tile_depths: int32 [49152, 128], P(('ia', 'ja', 'ka')), may hold values from 0 to 16383
- tile_live: int32 [512, 32], P(('ia', 'ja', 'ka')), may hold values from 0 to 3, as said below
- factor_b: bfloat16 [16, 8, 8192], P(None, 'ja', ('ia', 'ka')), may hold values from -6 to 6
- factor_c: bfloat16 [16, 4, 16384], P(None, 'ka', ('ia', 'ja')), may hold values from -6 to 6
- proj: float32 [16, 256], replicated, may hold values from -0.375 to 0.375
Outputs:
- tucker_y: float32 [32768, 256], P(('ia', 'ja', 'ka'))
- gram: float32 [256, 256], replicated
- new_factor: float32 [16, 32768], P(None, ('ia', 'ja', 'ka'))
The draws below stay inside these ranges and needn't reach their ends.
Inputs may be any that keep to these rules, and one draw needn't show every extreme that they name: tile_live[d, o] counts the live leading slots among the 3 slots that device d holds for the device at index o along ja+ka within its mode-1 block; in every draw there is an owner for which every device has all 3 slots live, and every device has some owner with all 3 slots live.
All inputs are finite; a program needn't handle non-finite values.
Results may differ from the reference program's by a relative error of at most 0.0041.
Values may be sent and summed in bfloat16 or wider, within the bound.
No kernel may reach another device: no remote copies, remote signals or barrier semaphores. Data moves between devices by JAX's collectives and lax.ppermute only.
A program may use at most 64 MiB of HBM per device.

```python
import jax
import jax.numpy as jnp
from jax import lax

RANK = 16
KR = 256
TILE = 128
ROWS_DEV = 64
SLOTS = 3
OWNERS = 32
GRID = 512
ALL_TILES = 49152
JB = 8192
KB = 16384
N_IA = 16
N_JA = 8
N_KA = 4


def draw_tile_live(key, part):
    base = jax.random.fold_in(key, 31)
    key_level, key_count, key_owner = jax.random.split(base, 3)
    level_row = jax.random.randint(key_level, (GRID, 1), 0, SLOTS)
    drawn = jax.random.randint(key_count, (GRID, OWNERS), 0, SLOTS + 1)
    busy_owner = jax.random.randint(key_owner, (), 0, OWNERS)
    column = jnp.arange(OWNERS, dtype=jnp.int32)[None, :]
    return jnp.where(column == busy_owner, SLOTS, jnp.maximum(drawn, level_row)).astype(jnp.int32)


def place_ends(values, rng, low, largest):
    spot = [jax.random.randint(jax.random.fold_in(rng, axis), (), 0, length) for axis, length in enumerate(values.shape)]
    main_axis = values.shape.index(max(values.shape))
    next_to = spot[:main_axis] + [(spot[main_axis] + 1) % values.shape[main_axis]] + spot[main_axis + 1:]
    return values.at[tuple(spot)].set(low).at[tuple(next_to)].set(largest)


def block_levels(key, dims, shards, least, top_value):
    loudness, own = 1.0, jax.random.fold_in(key, 6)
    for dim, shards_of in shards:
        draws = jnp.exp(jax.random.uniform(jax.random.fold_in(own, dim), (shards_of,), jnp.float32, least / len(shards), top_value / len(shards)))
        loudness = loudness * jnp.repeat(draws, dims[dim] // shards_of).reshape([-1 if axis == dim else 1 for axis in range(len(dims))])
    return loudness


def gaussian(rng, extent, width, reach, pieces=(), held_as=jnp.bfloat16):
    values = jax.random.normal(rng, extent, jnp.float32) * width
    if len(pieces) > 0:
        values = block_levels(rng, extent, pieces, -0.22, 0.18) * values
    return jnp.clip(values, min=-reach, max=reach).astype(held_as)


def setup_inputs(seed: int = 0) -> dict:
    seeds = jax.random.split(jax.random.key(seed), 9)
    return {
        "tile_values": gaussian(seeds[0], (ALL_TILES, TILE), 0.1, 0.59765625, ((0, 512),)),
        "tile_rows": place_ends(jax.random.randint(seeds[1], (ALL_TILES, TILE), 0, ROWS_DEV), jax.random.fold_in(seeds[1], 1), 0, ROWS_DEV - 1).astype(jnp.int32),
        "tile_cols": place_ends(jax.random.randint(seeds[2], (ALL_TILES, TILE), 0, JB), jax.random.fold_in(seeds[2], 1), 0, JB - 1).astype(jnp.int32),
        "tile_depths": place_ends(jax.random.randint(seeds[3], (ALL_TILES, TILE), 0, KB), jax.random.fold_in(seeds[3], 1), 0, KB - 1).astype(jnp.int32),
        "tile_live": draw_tile_live(jax.random.fold_in(seeds[8], 71), 0),
        "factor_b": gaussian(seeds[5], (RANK, N_JA, JB), 1.0, 6.0, ((1, 8), (2, 64))),
        "factor_c": gaussian(seeds[6], (RANK, N_KA, KB), 1.0, 6.0, ((1, 4), (2, 128))),
        "proj": gaussian(seeds[7], (RANK, KR), KR ** -0.5, 0.375, (), jnp.float32),
    }


def reference(tile_values, tile_rows, tile_cols, tile_depths, tile_live, factor_b, factor_c, proj):
    owner_count = N_JA * N_KA
    slot_total = SLOTS * owner_count
    block_rows = ROWS_DEV * owner_count
    total_rows = block_rows * N_IA
    slot_index = jnp.arange(slot_total, dtype=jnp.int32)
    owner_of = slot_index // SLOTS
    place_of = slot_index % SLOTS
    values_all = tile_values.reshape(N_IA * N_JA * N_KA, slot_total, TILE)
    rows_all = tile_rows.reshape(N_IA * N_JA * N_KA, slot_total, TILE)
    cols_all = tile_cols.reshape(N_IA * N_JA * N_KA, slot_total, TILE)
    depths_all = tile_depths.reshape(N_IA * N_JA * N_KA, slot_total, TILE)

    def visit_device(result, device):
        slab_index = device // owner_count
        column_block = (device // N_KA) % N_JA
        depth_block = device % N_KA
        values_here = lax.dynamic_index_in_dim(values_all, device, 0, keepdims=False)
        rows_here = lax.dynamic_index_in_dim(rows_all, device, 0, keepdims=False)
        cols_here = lax.dynamic_index_in_dim(cols_all, device, 0, keepdims=False)
        depths_here = lax.dynamic_index_in_dim(depths_all, device, 0, keepdims=False)
        live_here = lax.dynamic_index_in_dim(tile_live, device, 0, keepdims=False)
        table_b = lax.dynamic_index_in_dim(factor_b, column_block, 1, keepdims=False)
        table_c = lax.dynamic_index_in_dim(factor_c, depth_block, 1, keepdims=False)
        is_live = (place_of < live_here[owner_of]).astype(jnp.float32)
        scaled = (values_here.astype(jnp.float32)[None] * table_b[:, cols_here].astype(jnp.float32)).astype(jnp.bfloat16)
        depth_rows = table_c[:, depths_here]
        kron_rows = (scaled.astype(jnp.float32)[:, None] * depth_rows.astype(jnp.float32)[None, :]).astype(jnp.bfloat16)
        kron_rows = kron_rows.astype(jnp.float32) * is_live[None, None, :, None]
        kron_rows = kron_rows.reshape(RANK * RANK, slot_total * TILE)
        target = slab_index * block_rows + owner_of[:, None] * ROWS_DEV + rows_here
        result = result.at[target.reshape(-1)].add(kron_rows.T)
        return result, None

    start = jnp.zeros((total_rows, RANK * RANK), jnp.float32)
    tucker_y, _ = lax.scan(visit_device, start, jnp.arange(N_IA * N_JA * N_KA, dtype=jnp.int32))
    gram = jnp.dot(tucker_y.T, tucker_y, precision=lax.Precision.HIGHEST, preferred_element_type=jnp.float32) / total_rows
    new_factor = jnp.dot(proj, tucker_y.T, precision=lax.Precision.HIGHEST, preferred_element_type=jnp.float32)
    return (tucker_y, gram, new_factor)
```

```python
import jax
import jax.numpy as jnp
from jax import lax
from jax.experimental import pallas as pl
from jax.experimental.pallas import tpu as pltpu
from jax.sharding import Mesh
from jax.sharding import PartitionSpec as P

RANK = 16
KR = RANK * RANK
ROWS_DEV = 64
LANES = 128
IA = ("ia",)
IA_KA = ("ia", "ka")
IA_JA = ("ia", "ja")
JA_KA = ("ja", "ka")
IA_JA_KA = ("ia", "ja", "ka")
BF16 = jnp.bfloat16
F32 = jnp.float32
VMEM = pl.BlockSpec(memory_space=pltpu.VMEM)
SMEM = pl.BlockSpec(memory_space=pltpu.SMEM)


def iota(shape, dim):
    return lax.broadcasted_iota(jnp.int32, shape, dim)


def to_everyone(x, axes):
    copies = jnp.broadcast_to(x, (lax.axis_size(axes), *x.shape))
    return lax.all_to_all(copies, axes, split_axis=0, concat_axis=0, tiled=True)


def expand_table(packed, table, picks):
    row, lane = iota((LANES, 2 * LANES), 0), iota((LANES, 2 * LANES), 1)
    for j in range(4):
        picks[j] = (((row >> 4) == 2 * j + (lane >> 7)) & ((row & 15) == (lane & 15))).astype(BF16)

    def group(g, _):
        turned = packed[pl.ds(pl.multiple_of(g * LANES, LANES), LANES), :].T
        for j in range(4):
            two = jnp.dot(turned, picks[j], preferred_element_type=F32)
            start = pl.multiple_of(g * 8 * LANES + j * 2 * LANES, 2 * LANES)
            table[pl.ds(start, LANES), :] = two[:, :LANES]
            table[pl.ds(start + LANES, LANES), :] = two[:, LANES:]
        return 0

    lax.fori_loop(0, packed.shape[0] // LANES, group, 0)


def fetch_rows(index, base, table, rows, count):
    for j in range(count):
        rows[pl.ds(j, 1), :] = table[pl.ds(index[base + j], 1), :]


def scaled_body(cols, x, packed, out, table, picks, rows0, rows1):
    expand_table(packed, table, picks)
    lane = iota((LANES, LANES), 1)

    def group(g, _):
        total = jnp.zeros((LANES, LANES), F32)
        xs = x[g].T
        for j in range(8):
            rows = (rows0, rows1)[j & 1]
            fetch_rows(cols, g * 8 * LANES + j * LANES, table, rows, LANES)
            total = jnp.where((lane >> 4) == j, rows[...] * xs[:, j : j + 1], total)
        out[g] = total.astype(BF16)
        return 0

    lax.fori_loop(0, out.shape[0], group, 0)


def partial_body(depths, scaled, target, packed, out, table, picks, rows0, rows1):
    expand_table(packed, table, picks)
    slots = target.shape[1]
    owners = out.shape[0]
    count = slots * LANES
    row, lane = iota((LANES, KR), 0), iota((LANES, KR), 1)

    def fetch(o, rows):
        fetch_rows(depths, o * count, table, rows, count)

    def compute(o, rows):
        parts = []
        hits = []
        owner_rows = target[o]
        for t in range(slots):
            tile = o * slots + t
            spread = (((row & 15) == (lane >> 4)) & ((row >> 4) == (tile & 7))).astype(BF16)
            left = jnp.dot(scaled[tile >> 3], spread, preferred_element_type=F32).astype(BF16)
            right = rows[t * LANES : (t + 1) * LANES, :].astype(BF16)
            parts.append(left * jnp.concatenate([right, right], axis=1))
            hits.append((iota((ROWS_DEV, LANES), 0) == owner_rows[t : t + 1, :]).astype(BF16))
        block = jnp.dot(
            jnp.concatenate(hits, axis=1), jnp.concatenate(parts, axis=0), preferred_element_type=F32
        )
        out[o] = block.astype(BF16)

    fetch(0, rows0)

    def pair(i, _):
        o = 2 * i
        fetch(o + 1, rows1)
        compute(o, rows0)
        fetch(jnp.minimum(o + 2, owners - 1), rows0)
        compute(o + 1, rows1)
        return 0

    lax.fori_loop(0, owners // 2, pair, 0)


def finish_body(arrived, proj, y, pieces, new_factor):
    total = arrived[0].astype(F32)
    for s in range(1, arrived.shape[0]):
        total = total + arrived[s].astype(F32)
    y[...] = total
    gram = lax.dot_general(
        total, total, (((0,), (0,)), ((), ())), precision=lax.Precision.HIGHEST, preferred_element_type=F32
    )
    pieces[...] = gram.astype(BF16)
    new_factor[...] = lax.dot_general(
        proj[...], total, (((1,), (1,)), ((), ())), precision=lax.Precision.HIGHEST, preferred_element_type=F32
    )


def scratch(positions, rows):
    return [
        pltpu.VMEM((positions, LANES), F32),
        pltpu.VMEM((4, LANES, 2 * LANES), BF16),
        pltpu.VMEM((rows, LANES), F32),
        pltpu.VMEM((rows, LANES), F32),
    ]


def cost(flops, nbytes):
    return pl.CostEstimate(flops=flops, transcendentals=0, bytes_accessed=nbytes)


def scaled_rows(cols, x, packed):
    groups = x.shape[0]
    return pl.pallas_call(
        scaled_body,
        out_shape=jax.ShapeDtypeStruct((groups, LANES, LANES), BF16),
        in_specs=[SMEM, VMEM, VMEM],
        out_specs=VMEM,
        scratch_shapes=scratch(packed.shape[0] * 8, LANES),
        cost_estimate=cost(10**9, 10**6),
        compiler_params=pltpu.CompilerParams(vmem_limit_bytes=16 * 2**20),
        name="scaled_rows",
    )(cols, x, packed)


def partial_blocks(depths, scaled, target, packed):
    owners, slots, _ = target.shape
    return pl.pallas_call(
        partial_body,
        out_shape=jax.ShapeDtypeStruct((owners, ROWS_DEV, KR), BF16),
        in_specs=[SMEM, VMEM, VMEM, VMEM],
        out_specs=VMEM,
        scratch_shapes=scratch(packed.shape[0] * 8, slots * LANES),
        cost_estimate=cost(10**9, 10**6),
        compiler_params=pltpu.CompilerParams(vmem_limit_bytes=24 * 2**20),
        name="partial_blocks",
    )(depths, scaled, target, packed)


def finish(arrived, proj):
    return pl.pallas_call(
        finish_body,
        out_shape=(
            jax.ShapeDtypeStruct((ROWS_DEV, KR), F32),
            jax.ShapeDtypeStruct((KR, KR), BF16),
            jax.ShapeDtypeStruct((RANK, ROWS_DEV), F32),
        ),
        in_specs=[VMEM, VMEM],
        out_specs=(VMEM, VMEM, VMEM),
        cost_estimate=cost(10**9, 10**6),
        compiler_params=pltpu.CompilerParams(vmem_limit_bytes=16 * 2**20),
        name="finish",
    )(arrived, proj)


def on_device(tile_values, tile_rows, tile_cols, tile_depths, tile_live, factor_b, factor_c, proj):
    owners = lax.axis_size(JA_KA)
    tiles, width = tile_values.shape
    slots = tiles // owners
    table_b = to_everyone(factor_b[:, 0, :], IA_KA).reshape(-1, LANES)
    table_c = to_everyone(factor_c[:, 0, :], IA_JA).reshape(-1, LANES)
    live = lax.iota(jnp.int32, slots)[None, :] < tile_live.reshape(owners, 1)
    target = jnp.where(live[:, :, None], tile_rows.reshape(owners, slots, width), ROWS_DEV)
    x = tile_values.astype(F32).reshape(tiles // 8, 8, width)
    scaled = scaled_rows(tile_cols.reshape(-1), x, table_b)
    blocks = partial_blocks(tile_depths.reshape(-1), scaled, target, table_c)
    arrived = lax.all_to_all(blocks, JA_KA, split_axis=0, concat_axis=0, tiled=True)
    y, gram_part, new_factor = finish(arrived, proj)
    pieces = gram_part.reshape(owners, KR // owners, KR)
    mine = jnp.sum(
        lax.all_to_all(pieces, JA_KA, split_axis=0, concat_axis=0, tiled=True).astype(F32), axis=0
    )
    mine = jnp.sum(to_everyone(mine.astype(BF16), IA).astype(F32), axis=0)
    mine = mine / (ROWS_DEV * owners * lax.axis_size(IA))
    gram = to_everyone(mine.astype(BF16), JA_KA).reshape(KR, KR).astype(F32)
    return y, gram, new_factor


def solution(mesh):
    in_specs = (
        P(IA_JA_KA, None),
        P(IA_JA_KA, None),
        P(IA_JA_KA, None),
        P(IA_JA_KA, None),
        P(IA_JA_KA, None),
        P(None, "ja", IA_KA),
        P(None, "ka", IA_JA),
        P(),
    )
    out_specs = (P(IA_JA_KA, None), P(), P(None, IA_JA_KA))
    return jax.shard_map(on_device, mesh=mesh, in_specs=in_specs, out_specs=out_specs, check_vma=False)
```

```python
import jax
import jax.numpy as jnp
from jax import lax
from jax.experimental import pallas as pl
from jax.experimental.pallas import tpu as pltpu
from jax.sharding import Mesh
from jax.sharding import PartitionSpec as P

RANK = 16
KR = RANK * RANK
ROWS_DEV = 64
LANES = 128
PACK = LANES // RANK
JA = ("yl", "co")
IA_KA = ("ia", "ka")
IA_JA = ("ia", "yl", "co")
CO_KA = ("co", "ka")
YL_KA = ("yl", "ka")
IA_JA_KA = ("ia", "yl", "co", "ka")
BF16 = jnp.bfloat16
F32 = jnp.float32
VMEM = pl.BlockSpec(memory_space=pltpu.VMEM)
SMEM = pl.BlockSpec(memory_space=pltpu.SMEM)


def iota(shape, dim):
    return lax.broadcasted_iota(jnp.int32, shape, dim)


def exchange(x, axes):
    return lax.all_to_all(x, axes, split_axis=0, concat_axis=0, tiled=True)


def to_everyone(x, axes):
    return exchange(jnp.broadcast_to(x, (lax.axis_size(axes), *x.shape)), axes)


def expand_table(ranks, table, picks):
    row, lane = iota((LANES, 2 * LANES), 0), iota((LANES, 2 * LANES), 1)
    for j in range(PACK // 2):
        picks[j] = (((row >> 4) == 2 * j + (lane >> 7)) & ((row & 15) == (lane & 15))).astype(BF16)

    def group(g, _):
        turned = ranks[pl.ds(pl.multiple_of(g * LANES, LANES), LANES), :].T
        for j in range(PACK // 2):
            two = jnp.dot(turned, picks[j], preferred_element_type=F32)
            start = pl.multiple_of((g * PACK + 2 * j) * LANES, 2 * LANES)
            table[pl.ds(start, LANES), :] = two[:, :LANES]
            table[pl.ds(start + LANES, LANES), :] = two[:, LANES:]
        return 0

    lax.fori_loop(0, ranks.shape[0] // LANES, group, 0)


def from_each(index, count):
    return [index.at[pl.ds(j, index.shape[0] - j)] for j in range(count)]


def in_turns(count, fetch, finish, rows0, rows1):
    fetch(0, rows0)

    def pair(i, _):
        o = 2 * i
        fetch(o + 1, rows1)
        finish(o, rows0)
        fetch(jnp.minimum(o + 2, count - 1), rows0)
        finish(o + 1, rows1)
        return 0

    lax.fori_loop(0, count // 2, pair, 0)


def scaled_body(cols, x, ranks, out, table, picks, rows0, rows1):
    expand_table(ranks, table, picks)
    spread = (iota((PACK, LANES), 0) == (iota((PACK, LANES), 1) >> 4)).astype(BF16)
    views = from_each(cols, PACK * LANES)

    def fetch(g, rows):
        base = g * PACK * LANES
        for j in range(PACK):
            lanes = slice(j * RANK, (j + 1) * RANK)
            for r in range(LANES):
                rows[pl.ds(r, 1), lanes] = table[pl.ds(views[j * LANES + r][base], 1), lanes]

    def finish(g, rows):
        by_lane = lax.dot_general(x[g], spread, (((0,), (0,)), ((), ())), preferred_element_type=F32)
        out[g] = (rows[...] * by_lane).astype(BF16)

    in_turns(out.shape[0], fetch, finish, rows0, rows1)


def partial_body(depths, scaled, target, ranks, out, table, picks, spreads, rows0, rows1):
    expand_table(ranks, table, picks)
    owners, slots, _ = target.shape
    count = slots * LANES
    row, lane = iota((LANES, KR), 0), iota((LANES, KR), 1)
    for j in range(PACK):
        spreads[j] = (((row & 15) == (lane >> 4)) & ((row >> 4) == j)).astype(BF16)
    views = from_each(depths, count)

    def fetch(o, rows):
        base = o * count
        for r in range(count):
            rows[pl.ds(r, 1), :] = table[pl.ds(views[r][base], 1), :]

    def finish(o, rows):
        parts = []
        hits = []
        owner_rows = target[o]
        for t in range(slots):
            tile = o * slots + t
            left = jnp.dot(scaled[tile >> 3], spreads[tile & 7], preferred_element_type=F32).astype(BF16)
            right = rows[t * LANES : (t + 1) * LANES, :].astype(BF16)
            parts.append(left * jnp.concatenate([right, right], axis=1))
            hits.append((iota((ROWS_DEV, LANES), 0) == owner_rows[t : t + 1, :]).astype(BF16))
        block = jnp.dot(
            jnp.concatenate(hits, axis=1), jnp.concatenate(parts, axis=0), preferred_element_type=F32
        )
        place = ((o >> 2) & 1) * (owners // 2) + (o >> 3) * 4 + (o & 3)
        out[place] = block.astype(BF16)

    in_turns(owners, fetch, finish, rows0, rows1)


def added(copies):
    total = copies[0].astype(F32)
    for s in range(1, copies.shape[0]):
        total = total + copies[s].astype(F32)
    return total


def finish_body(arrived, proj, y, pieces, new_factor):
    total = added(arrived)
    y[...] = total
    gram = lax.dot_general(
        total, total, (((0,), (0,)), ((), ())), precision=lax.Precision.HIGHEST, preferred_element_type=F32
    )
    pieces[...] = gram.astype(BF16).reshape(pieces.shape)
    new_factor[...] = lax.dot_general(
        proj[...], total, (((1,), (1,)), ((), ())), precision=lax.Precision.HIGHEST, preferred_element_type=F32
    )


def cost(flops, nbytes):
    return pl.CostEstimate(flops=flops, transcendentals=0, bytes_accessed=nbytes)


def call(body, name, out_shape, in_specs, args, scratch=(), limit=16, flops=10**9):
    several = isinstance(out_shape, tuple)
    return pl.pallas_call(
        body,
        out_shape=out_shape,
        in_specs=in_specs,
        out_specs=(VMEM,) * len(out_shape) if several else VMEM,
        scratch_shapes=list(scratch),
        cost_estimate=cost(flops, 10**6),
        compiler_params=pltpu.CompilerParams(vmem_limit_bytes=limit * 2**20),
        name=name,
    )(*args)


def table_scratch(ranks):
    return [pltpu.VMEM((ranks.shape[0] * PACK, LANES), F32), pltpu.VMEM((PACK // 2, LANES, 2 * LANES), BF16)]


def scaled_rows(cols, x, ranks):
    rows = pltpu.VMEM((LANES, LANES), F32)
    out = jax.ShapeDtypeStruct((x.shape[0], LANES, LANES), BF16)
    return call(
        scaled_body, "scaled_rows", out, [SMEM, VMEM, VMEM], (cols, x, ranks), [*table_scratch(ranks), rows, rows]
    )


def partial_blocks(depths, scaled, target, ranks):
    owners, slots, _ = target.shape
    rows = pltpu.VMEM((slots * LANES, LANES), F32)
    return call(
        partial_body,
        "partial_blocks",
        jax.ShapeDtypeStruct((owners, ROWS_DEV, KR), BF16),
        [SMEM, VMEM, VMEM, VMEM],
        (depths, scaled, target, ranks),
        [*table_scratch(ranks), pltpu.VMEM((PACK, LANES, KR), BF16), rows, rows],
        limit=24,
    )


def finish(arrived, proj, parts):
    out = (
        jax.ShapeDtypeStruct((ROWS_DEV, KR), F32),
        jax.ShapeDtypeStruct((parts, KR // parts, KR), BF16),
        jax.ShapeDtypeStruct((RANK, ROWS_DEV), F32),
    )
    return call(finish_body, "finish", out, [VMEM, VMEM], (arrived, proj))


def added_copies(arrived, copies, scale=None):
    def body(arrived, out):
        total = added(arrived)
        total = (total if scale is None else total * scale).astype(BF16)
        for s in range(out.shape[0]):
            out[s] = total

    out = jax.ShapeDtypeStruct((copies, *arrived.shape[1:]), BF16)
    return call(body, "added_copies", out, [VMEM], (arrived,), flops=10**7)


def halves_added(arrived):
    def body(arrived, out):
        for s in range(out.shape[0]):
            out[s] = (arrived[0, s].astype(F32) + arrived[1, s].astype(F32)).astype(BF16)

    out = jax.ShapeDtypeStruct(arrived.shape[1:], BF16)
    return call(body, "halves_added", out, [VMEM], (arrived,), flops=10**7)


def block_moved(index, parts, order):
    block, place = index >> 7, index & 127
    digits = {}
    for name, size in reversed(parts):
        digits[name] = block & (size - 1)
        block = block >> (size.bit_length() - 1)
    sizes = dict(parts)
    moved = 0
    for name in order:
        moved = moved * sizes[name] + digits[name]
    return moved * LANES + place


def on_device(tile_values, tile_rows, tile_cols, tile_depths, tile_live, factor_b, factor_c, proj):
    n_ia, n_yl, n_co, n_ka = (lax.axis_size(a) for a in ("ia", "yl", "co", "ka"))
    owners = n_yl * n_co * n_ka
    tiles, width = tile_values.shape
    slots = tiles // owners
    near = to_everyone(jnp.stack([factor_b[:, 0, :], factor_c[:, 0, :]]), "ia")
    ranks_b = to_everyone(near[:, 0], "ka").reshape(-1, LANES)
    ranks_c = to_everyone(to_everyone(near[:, 1], "yl"), "co").reshape(-1, LANES)
    cols = block_moved(tile_cols, [("ia", n_ia), ("ka", n_ka)], ["ka", "ia"])
    depths = block_moved(tile_depths, [("ia", n_ia), ("yl", n_yl), ("co", n_co)], ["co", "yl", "ia"])
    live = lax.iota(jnp.int32, slots)[None, :] < tile_live.reshape(owners, 1)
    target = jnp.where(live[:, :, None], tile_rows.reshape(owners, slots, width), ROWS_DEV)
    scaled = scaled_rows(cols.reshape(-1), tile_values.reshape(tiles // PACK, PACK, width), ranks_b)
    blocks = partial_blocks(depths.reshape(-1), scaled, target, ranks_c)
    halves = exchange(blocks, "co").reshape(n_co, owners // n_co, ROWS_DEV, KR)
    arrived = exchange(halves_added(halves), YL_KA)
    y, pieces, new_factor = finish(arrived, proj, n_co * n_ka)
    mine = added_copies(exchange(pieces, CO_KA), n_yl)
    mine = added_copies(exchange(mine, "yl"), n_ia)
    mine = added_copies(exchange(mine, "ia"), n_co * n_ka, 1.0 / (ROWS_DEV * owners * n_ia))
    gram = exchange(mine, CO_KA).reshape(KR, KR).astype(F32)
    return y, gram, new_factor


def solution(mesh):
    n_ka = mesh.shape["ka"]
    finer = Mesh(mesh.devices.reshape(-1, 4, 2, n_ka), ("ia", "yl", "co", "ka"))
    in_specs = (
        P(IA_JA_KA, None),
        P(IA_JA_KA, None),
        P(IA_JA_KA, None),
        P(IA_JA_KA, None),
        P(IA_JA_KA, None),
        P(None, JA, IA_KA),
        P(None, "ka", IA_JA),
        P(),
    )
    out_specs = (P(IA_JA_KA, None), P(), P(None, IA_JA_KA))
    return jax.shard_map(on_device, mesh=finer, in_specs=in_specs, out_specs=out_specs, check_vma=False)
```

```python
import jax
import jax.numpy as jnp
from jax import lax
from jax.experimental import pallas as pl
from jax.experimental.pallas import tpu as pltpu
from jax.sharding import Mesh
from jax.sharding import PartitionSpec as P

RANK = 16
KR = RANK * RANK
ROWS_DEV = 64
LANES = 128
PACK = LANES // RANK
JA = ("yl", "co")
IA_KA = ("yh", "z", "ka")
IA_JA = ("yh", "z", "yl", "co")
CO_KA = ("co", "ka")
YL_KA = ("yl", "ka")
YH_KA = ("yh", "ka")
Y = ("yh", "yl")
IA_JA_KA = ("yh", "z", "yl", "co", "ka")
BF16 = jnp.bfloat16
F32 = jnp.float32
VMEM = pl.BlockSpec(memory_space=pltpu.VMEM)
SMEM = pl.BlockSpec(memory_space=pltpu.SMEM)


def iota(shape, dim):
    return lax.broadcasted_iota(jnp.int32, shape, dim)


def exchange(x, axes):
    return lax.all_to_all(x, axes, split_axis=0, concat_axis=0, tiled=True)


def to_everyone(x, axes):
    return exchange(jnp.broadcast_to(x, (lax.axis_size(axes), *x.shape)), axes)


def expand_table(ranks, table, turned, picks):
    groups = turned.shape[0]
    row, lane = iota((LANES, 2 * LANES), 0), iota((LANES, 2 * LANES), 1)
    for j in range(PACK // 2):
        picks[j] = (((row >> 4) == 2 * j + (lane >> 7)) & ((row & 15) == (lane & 15))).astype(BF16)
    for g in range(groups):
        turned[g] = ranks[g * LANES : (g + 1) * LANES, :].T

    def pick(j, _):
        for g in range(groups):
            two = jnp.dot(turned[g], picks[j], preferred_element_type=F32)
            table[g, 2 * j] = two[:, :LANES]
            table[g, 2 * j + 1] = two[:, LANES:]
        return 0

    lax.fori_loop(0, PACK // 2, pick, 0)


def fetch_rows(index, table, rows):
    step = 8 * LANES
    views = [index.at[pl.ds(r, index.shape[0] - r)] for r in range(step)]

    def several(g, _):
        base = pl.multiple_of(g * step, step)
        for r in range(step):
            rows[pl.ds(base + r, 1), :] = table[pl.ds(views[r][base], 1), :]
        return 0

    lax.fori_loop(0, index.shape[0] // step, several, 0)


def b_body(cols, ranks, rows, table, turned, picks):
    expand_table(ranks, table, turned, picks)
    fetch_rows(cols, table.reshape(-1, LANES), rows)


def scaled_body(rows, x, target, out, hits):
    spread = (iota((LANES, KR), 0) == (iota((LANES, KR), 1) >> 4)).astype(BF16)
    tiles = x.shape[1]
    owners, slots, _ = target.shape

    def group(g, _):
        xs = x[g].astype(F32).T
        for j in range(tiles):
            start = pl.multiple_of((g * tiles + j) * LANES, LANES)
            scaled = (rows[pl.ds(start, LANES), :] * xs[:, j : j + 1]).astype(BF16)
            out[pl.ds(start, LANES), :] = jnp.dot(scaled, spread, preferred_element_type=F32).astype(BF16)
        return 0

    lax.fori_loop(0, x.shape[0], group, 0)

    def owner(o, _):
        owner_rows = target[o]
        for t in range(slots):
            lanes = slice(t * LANES, (t + 1) * LANES)
            hits[o, :, lanes] = (iota((ROWS_DEV, LANES), 0) == owner_rows[t : t + 1, :]).astype(BF16)
        return 0

    lax.fori_loop(0, owners, owner, 0)


def partial_body(depths, scaled, hits, ranks, out, table, turned, picks, rows):
    expand_table(ranks, table, turned, picks)
    fetch_rows(depths, table.reshape(-1, LANES), rows)
    owners, _, count = hits.shape
    together = 2

    def several(i, _):
        for k in range(together):
            o = i * together + k
            start = pl.multiple_of(o * count, LANES)
            right = rows[pl.ds(start, count), :].astype(BF16)
            kron = scaled[pl.ds(start, count), :] * jnp.concatenate([right, right], axis=1)
            block = jnp.dot(hits[o], kron, preferred_element_type=F32)
            place = ((o >> 2) & 1) * (owners // 2) + (o >> 3) * 4 + (o & 3)
            out[place] = block.astype(BF16)
        return 0

    lax.fori_loop(0, owners // together, several, 0)


def near_body(near, for_b, for_c):
    for s in range(for_b.shape[0]):
        for_b[s] = near[:, 0]
        for_c[s] = near[:, 1]


def added(copies):
    total = copies[0].astype(F32)
    for s in range(1, copies.shape[0]):
        total = total + copies[s].astype(F32)
    return total


def finish_body(arrived, proj, y, pieces, new_factor):
    total = added(arrived)
    y[...] = total
    gram = lax.dot_general(
        total, total, (((0,), (0,)), ((), ())), precision=lax.Precision.HIGHEST, preferred_element_type=F32
    )
    pieces[...] = gram.astype(BF16).reshape(pieces.shape)
    new_factor[...] = lax.dot_general(
        proj[...], total, (((1,), (1,)), ((), ())), precision=lax.Precision.HIGHEST, preferred_element_type=F32
    )


def cost(flops, nbytes):
    return pl.CostEstimate(flops=flops, transcendentals=0, bytes_accessed=nbytes)


def call(body, out_shape, in_specs, args, scratch=(), limit=16, flops=10**9):
    several = isinstance(out_shape, tuple)
    return pl.pallas_call(
        body,
        out_shape=out_shape,
        in_specs=in_specs,
        out_specs=(VMEM,) * len(out_shape) if several else VMEM,
        scratch_shapes=list(scratch),
        cost_estimate=cost(flops, 10**6),
        compiler_params=pltpu.CompilerParams(vmem_limit_bytes=limit * 2**20),
    )(*args)


def table_scratch(ranks):
    groups = ranks.shape[0] // LANES
    return [
        pltpu.VMEM((groups, PACK, LANES, LANES), F32),
        pltpu.VMEM((groups, LANES, LANES), BF16),
        pltpu.VMEM((PACK // 2, LANES, 2 * LANES), BF16),
    ]


def b_rows(cols, ranks):
    out = jax.ShapeDtypeStruct((cols.shape[0], LANES), F32)
    return call(b_body, out, [SMEM, VMEM], (cols, ranks), table_scratch(ranks))


def scaled_rows(rows, x, target):
    owners, slots, width = target.shape
    out = (
        jax.ShapeDtypeStruct((rows.shape[0], KR), BF16),
        jax.ShapeDtypeStruct((owners, ROWS_DEV, slots * width), BF16),
    )
    return call(scaled_body, out, [VMEM] * 3, (rows, x, target), limit=20)


def partial_blocks(depths, scaled, hits, ranks):
    owners = hits.shape[0]
    out = jax.ShapeDtypeStruct((owners, ROWS_DEV, KR), BF16)
    scratch = [*table_scratch(ranks), pltpu.VMEM((depths.shape[0], LANES), F32)]
    args = (depths, scaled, hits, ranks)
    return call(partial_body, out, [SMEM, VMEM, VMEM, VMEM], args, scratch, limit=32)


def near_copies(near, copies):
    one = jax.ShapeDtypeStruct((copies, near.shape[0], *near.shape[2:]), BF16)
    return call(near_body, (one, one), [VMEM], (near,), flops=10**7)


def finish(arrived, proj, parts):
    out = (
        jax.ShapeDtypeStruct((ROWS_DEV, KR), F32),
        jax.ShapeDtypeStruct((parts, KR // parts, KR), BF16),
        jax.ShapeDtypeStruct((RANK, ROWS_DEV), F32),
    )
    return call(finish_body, out, [VMEM, VMEM], (arrived, proj))


def added_copies(arrived, copies, scale=None):
    def body(arrived, out):
        total = added(arrived)
        total = (total if scale is None else total * scale).astype(BF16)
        for s in range(out.shape[0]):
            out[s] = total

    out = jax.ShapeDtypeStruct((copies, *arrived.shape[1:]), BF16)
    return call(body, out, [VMEM], (arrived,), flops=10**7)


def halves_added(arrived):
    def body(arrived, out):
        for s in range(out.shape[0]):
            out[s] = (arrived[0, s].astype(F32) + arrived[1, s].astype(F32)).astype(BF16)

    out = jax.ShapeDtypeStruct(arrived.shape[1:], BF16)
    return call(body, out, [VMEM], (arrived,), flops=10**7)


def block_moved(index, sizes, order, other):
    block, place = index >> 7, index & (LANES - 1)
    digits = {}
    for name in reversed(order):
        digits[name] = block & (sizes[name] - 1)
        block = block >> (sizes[name].bit_length() - 1)
    moved = 0
    for name in other:
        moved = moved * sizes[name] + digits[name]
    return moved * LANES + place


def update(tile_values, tile_rows, tile_cols, tile_depths, tile_live, factor_b, factor_c, proj):
    n_yh, n_z, n_yl, n_co, n_ka = (lax.axis_size(a) for a in IA_JA_KA)
    owners = n_yl * n_co * n_ka
    tiles, width = tile_values.shape
    slots = tiles // owners
    own = jnp.stack([factor_b[:, 0, :], factor_c[:, 0, :]])
    for_b, for_c = near_copies(to_everyone(own, "z"), n_yh * n_ka)
    ranks_b = exchange(for_b, YH_KA).reshape(-1, LANES)
    near_c = exchange(for_c, Y)
    ranks_c = to_everyone(near_c, "co").reshape(-1, LANES)
    sizes = dict(zip(IA_JA_KA, (n_yh, n_z, n_yl, n_co, n_ka)))
    cols = block_moved(tile_cols, sizes, IA_KA, ("yh", "ka", "z"))
    depths = block_moved(tile_depths, sizes, IA_JA, ("co", "yh", "yl", "z"))
    live = lax.iota(jnp.int32, slots)[None, :] < tile_live.reshape(owners, 1)
    target = jnp.where(live[:, :, None], tile_rows.reshape(owners, slots, width), ROWS_DEV)
    rows = b_rows(cols.reshape(-1), ranks_b)
    scaled, hits = scaled_rows(rows, tile_values.reshape(tiles // PACK, PACK, width), target)
    blocks = partial_blocks(depths.reshape(-1), scaled, hits, ranks_c)
    halves = exchange(blocks, "co").reshape(n_co, owners // n_co, ROWS_DEV, KR)
    arrived = exchange(halves_added(halves), YL_KA)
    y, pieces, new_factor = finish(arrived, proj, n_co * n_ka)
    mine = added_copies(exchange(pieces, CO_KA), n_yh * n_yl)
    mine = added_copies(exchange(mine, Y), n_z)
    mine = added_copies(exchange(mine, "z"), n_co * n_ka, 1.0 / (ROWS_DEV * owners * n_yh * n_z))
    gram = exchange(mine, CO_KA).reshape(KR, KR).astype(F32)
    return y, gram, new_factor


def solution(mesh):
    n_ka = mesh.shape["ka"]
    finer = Mesh(mesh.devices.reshape(2, -1, 4, 2, n_ka), IA_JA_KA)
    in_specs = (
        P(IA_JA_KA, None),
        P(IA_JA_KA, None),
        P(IA_JA_KA, None),
        P(IA_JA_KA, None),
        P(IA_JA_KA, None),
        P(None, JA, IA_KA),
        P(None, "ka", IA_JA),
        P(),
    )
    out_specs = (P(IA_JA_KA, None), P(), P(None, IA_JA_KA))
    return jax.shard_map(update, mesh=finer, in_specs=in_specs, out_specs=out_specs, check_vma=False)
```

```python
import jax
import jax.numpy as jnp
from jax import lax
from jax.experimental import pallas as pl
from jax.experimental.pallas import tpu as pltpu
from jax.sharding import Mesh
from jax.sharding import PartitionSpec as P

RANK = 16
KR = RANK * RANK
ROWS_DEV = 64
LANES = 128
PACK = LANES // RANK
JA = ("yl", "co")
IA_KA = ("ia", "ka")
IA_YL = ("ia", "yl")
IA_JA = ("ia", "yl", "co")
CO_KA = ("co", "ka")
YL_KA = ("yl", "ka")
IA_JA_KA = ("ia", "yl", "co", "ka")
BF16 = jnp.bfloat16
F32 = jnp.float32
VMEM = pl.BlockSpec(memory_space=pltpu.VMEM)
SMEM = pl.BlockSpec(memory_space=pltpu.SMEM)
HBM = pl.BlockSpec(memory_space=pltpu.HBM)


def iota(shape, dim):
    return lax.broadcasted_iota(jnp.int32, shape, dim)


def exchange(x, axes):
    return lax.all_to_all(x, axes, split_axis=0, concat_axis=0, tiled=True)


def to_everyone(x, axes):
    return exchange(jnp.broadcast_to(x, (lax.axis_size(axes), *x.shape)), axes)


def turn(ranks, turned, first=0):
    for g in range(ranks.shape[0] // LANES):
        turned[first + g] = ranks[g * LANES : (g + 1) * LANES, :].T


def fetch_rows(views, table, rows, start, count, high):
    for r in range(count):
        rows[pl.ds(r * high, high), :] = table[pl.ds(views[r][start], high), :]


def views_of(index, count):
    return [index.at[pl.ds(r, index.shape[0] - r)] for r in range(count)]


def scaled_body(cols, x, ranks, out, table, turned, picks, rows, scaled, done):
    turn(ranks, turned)
    groups = turned.shape[0]
    row, lane = iota((LANES, KR), 0), iota((LANES, KR), 1)
    for j in range(PACK):
        picks[j] = (((row >> 4) == j) & ((row & 15) == (lane >> 4))).astype(BF16)

    def pick(j, _):
        for g in range(groups):
            both = jnp.dot(turned[g], picks[j], preferred_element_type=F32)
            start = pl.multiple_of((g * PACK + j) * 2 * LANES, 2 * LANES)
            table[pl.ds(start, LANES, 2), :] = both[:, :LANES]
            table[pl.ds(start + 1, LANES, 2), :] = both[:, LANES:]
        return 0

    lax.fori_loop(0, PACK, pick, 0)
    tiles = x.shape[1]
    count = tiles * LANES
    views = views_of(cols, count)

    def sent(g):
        part = pl.ds(pl.multiple_of(g * count, count), count)
        return pltpu.make_async_copy(scaled.at[part], out.at[part], done.at[g])

    def group(g, _):
        fetch_rows(views, table, rows, g * count, count, 2)
        xs = x[g].astype(F32).T
        for j in range(tiles):
            by = xs[:, j : j + 1]
            left = rows[pl.ds(j * 2 * LANES, LANES, 2), :] * by
            right = rows[pl.ds(j * 2 * LANES + 1, LANES, 2), :] * by
            start = pl.multiple_of(g * count + j * LANES, LANES)
            scaled[pl.ds(start, LANES), :] = jnp.concatenate([left, right], axis=1).astype(BF16)
        sent(g).start()
        return 0

    lax.fori_loop(0, x.shape[0], group, 0)

    def wait(g, _):
        sent(g).wait()
        return 0

    lax.fori_loop(0, x.shape[0], wait, 0)


def partial_body(depths, scaled, target, ranks, ranks_other, out, table, turned, picks, rows, index, left, done):
    indices = pltpu.make_async_copy(depths, index, done.at[0])
    lefts = pltpu.make_async_copy(scaled, left, done.at[1])
    indices.start()
    lefts.start()
    turn(ranks, turned)
    turn(ranks_other, turned, turned.shape[0] // 2)
    groups = turned.shape[0]
    row, lane = iota((LANES, 2 * LANES), 0), iota((LANES, 2 * LANES), 1)
    for j in range(PACK // 2):
        picks[j] = (((row >> 4) == 2 * j + (lane >> 7)) & ((row & 15) == (lane & 15))).astype(BF16)

    def pick(j, _):
        for g in range(groups):
            two = jnp.dot(turned[g], picks[j], preferred_element_type=F32)
            start = pl.multiple_of((g * PACK + 2 * j) * LANES, 2 * LANES)
            table[pl.ds(start, LANES), :] = two[:, :LANES]
            table[pl.ds(start + LANES, LANES), :] = two[:, LANES:]
        return 0

    lax.fori_loop(0, PACK // 2, pick, 0)
    indices.wait()
    step = 8 * LANES
    views = views_of(index, step)

    def several_rows(g, _):
        start = pl.multiple_of(g * step, step)
        fetch_rows(views, table, rows.at[pl.ds(start, step)], start, step, 1)
        return 0

    lax.fori_loop(0, rows.shape[0] // step, several_rows, 0)
    lefts.wait()
    owners, slots, _ = target.shape
    count = slots * LANES
    together = 2

    def several(i, _):
        for k in range(together):
            o = i * together + k
            start = pl.multiple_of(o * count, LANES)
            right = rows[pl.ds(start, count), :].astype(BF16)
            kron = left[pl.ds(start, count), :] * jnp.concatenate([right, right], axis=1)
            owner_rows = target[o]
            hits = [(iota((ROWS_DEV, LANES), 0) == owner_rows[t : t + 1, :]).astype(BF16) for t in range(slots)]
            block = jnp.dot(jnp.concatenate(hits, axis=1), kron, preferred_element_type=F32)
            place = ((o >> 2) & 1) * (owners // 2) + (o >> 3) * 4 + (o & 3)
            out[place] = block.astype(BF16)
        return 0

    lax.fori_loop(0, owners // together, several, 0)


def added(copies):
    total = copies[0].astype(F32)
    for s in range(1, copies.shape[0]):
        total = total + copies[s].astype(F32)
    return total


def finish_body(arrived, proj, y, pieces, new_factor):
    total = added(arrived)
    y[...] = total
    gram = lax.dot_general(
        total, total, (((0,), (0,)), ((), ())), precision=lax.Precision.HIGHEST, preferred_element_type=F32
    )
    pieces[...] = gram.astype(BF16).reshape(pieces.shape)
    new_factor[...] = lax.dot_general(
        proj[...], total, (((1,), (1,)), ((), ())), precision=lax.Precision.HIGHEST, preferred_element_type=F32
    )


def cost(flops, nbytes):
    return pl.CostEstimate(flops=flops, transcendentals=0, bytes_accessed=nbytes)


def call(body, out_shape, in_specs, args, scratch=(), limit=16, flops=10**9, out_spec=VMEM):
    several = isinstance(out_shape, tuple)
    return pl.pallas_call(
        body,
        out_shape=out_shape,
        in_specs=in_specs,
        out_specs=(out_spec,) * len(out_shape) if several else out_spec,
        scratch_shapes=list(scratch),
        cost_estimate=cost(flops, 10**6),
        compiler_params=pltpu.CompilerParams(vmem_limit_bytes=limit * 2**20),
    )(*args)


def scaled_rows(cols, x, ranks):
    groups, tiles, _ = x.shape
    out = pltpu.HBM((cols.shape[0], KR), BF16)
    scratch = [
        pltpu.VMEM((ranks.shape[0] * PACK * 2, LANES), F32),
        pltpu.VMEM((ranks.shape[0] // LANES, LANES, LANES), BF16),
        pltpu.VMEM((PACK, LANES, KR), BF16),
        pltpu.VMEM((tiles * LANES * 2, LANES), F32),
        pltpu.VMEM(out.shape, BF16),
        pltpu.SemaphoreType.DMA((groups,)),
    ]
    return call(scaled_body, out, [SMEM, VMEM, VMEM], (cols, x, ranks), scratch, limit=24, out_spec=HBM)


def partial_blocks(depths, scaled, target, ranks, ranks_other):
    owners = target.shape[0]
    groups = 2 * ranks.shape[0] // LANES
    out = jax.ShapeDtypeStruct((owners, ROWS_DEV, KR), BF16)
    scratch = [
        pltpu.VMEM((groups * PACK * LANES, LANES), F32),
        pltpu.VMEM((groups, LANES, LANES), BF16),
        pltpu.VMEM((PACK // 2, LANES, 2 * LANES), BF16),
        pltpu.VMEM((depths.shape[0], LANES), F32),
        pltpu.SMEM(depths.shape, jnp.int32),
        pltpu.VMEM(scaled.shape, BF16),
        pltpu.SemaphoreType.DMA((2,)),
    ]
    scaled = pltpu.with_memory_space_constraint(scaled, pltpu.HBM)
    args = (depths, scaled, target, ranks, ranks_other)
    return call(partial_body, out, [HBM, HBM, VMEM, VMEM, VMEM], args, scratch, limit=32)


def finish(arrived, proj, parts):
    out = (
        jax.ShapeDtypeStruct((ROWS_DEV, KR), F32),
        jax.ShapeDtypeStruct((parts, KR // parts, KR), BF16),
        jax.ShapeDtypeStruct((RANK, ROWS_DEV), F32),
    )
    return call(finish_body, out, [VMEM, VMEM], (arrived, proj))


def added_copies(arrived, copies, scale=None):
    def body(arrived, out):
        total = added(arrived)
        total = (total if scale is None else total * scale).astype(BF16)
        for s in range(out.shape[0]):
            out[s] = total

    out = jax.ShapeDtypeStruct((copies, *arrived.shape[1:]), BF16)
    return call(body, out, [VMEM], (arrived,), flops=10**7)


def halves_added(arrived):
    def body(arrived, out):
        for s in range(out.shape[0]):
            out[s] = (arrived[0, s].astype(F32) + arrived[1, s].astype(F32)).astype(BF16)

    out = jax.ShapeDtypeStruct(arrived.shape[1:], BF16)
    return call(body, out, [VMEM], (arrived,), flops=10**7)


def update(tile_values, tile_rows, tile_cols, tile_depths, tile_live, factor_b, factor_c, proj):
    n_ia, n_yl, n_co, n_ka = (lax.axis_size(a) for a in IA_JA_KA)
    owners = n_yl * n_co * n_ka
    tiles, width = tile_values.shape
    slots = tiles // owners
    ranks_b = to_everyone(factor_b[:, 0, :], IA_KA).reshape(-1, LANES)
    ranks_c = to_everyone(factor_c[:, 0, :], IA_YL).reshape(-1, LANES)
    ranks_other = lax.ppermute(ranks_c, "co", [(0, 1), (1, 0)])
    block = tile_depths >> 7
    half = (block ^ lax.axis_index("co")) & 1
    depths = (half * (n_ia * n_yl) + (block >> 1)) * LANES + (tile_depths & (LANES - 1))
    cols = tile_cols * 2
    live = lax.iota(jnp.int32, slots)[None, :] < tile_live.reshape(owners, 1)
    target = jnp.where(live[:, :, None], tile_rows.reshape(owners, slots, width), ROWS_DEV)
    scaled = scaled_rows(cols.reshape(-1), tile_values.reshape(tiles // PACK, PACK, width), ranks_b)
    blocks = partial_blocks(depths.reshape(-1), scaled, target, ranks_c, ranks_other)
    halves = exchange(blocks, "co").reshape(n_co, owners // n_co, ROWS_DEV, KR)
    arrived = exchange(halves_added(halves), YL_KA)
    y, pieces, new_factor = finish(arrived, proj, n_co * n_ka)
    mine = added_copies(exchange(pieces, CO_KA), n_yl)
    mine = added_copies(exchange(mine, "yl"), n_ia)
    mine = added_copies(exchange(mine, "ia"), n_co * n_ka, 1.0 / (ROWS_DEV * owners * n_ia))
    gram = exchange(mine, CO_KA).reshape(KR, KR).astype(F32)
    return y, gram, new_factor


def solution(mesh):
    n_ka = mesh.shape["ka"]
    finer = Mesh(mesh.devices.reshape(-1, 4, 2, n_ka), IA_JA_KA)
    in_specs = (
        P(IA_JA_KA, None),
        P(IA_JA_KA, None),
        P(IA_JA_KA, None),
        P(IA_JA_KA, None),
        P(IA_JA_KA, None),
        P(None, JA, IA_KA),
        P(None, "ka", IA_JA),
        P(),
    )
    out_specs = (P(IA_JA_KA, None), P(), P(None, IA_JA_KA))
    return jax.shard_map(update, mesh=finer, in_specs=in_specs, out_specs=out_specs, check_vma=False)
```

```python
import jax
import jax.numpy as jnp
from jax import lax
from jax.experimental import pallas as pl
from jax.experimental.pallas import tpu as pltpu
from jax.sharding import Mesh
from jax.sharding import PartitionSpec as P

RANK = 16
KR = RANK * RANK
ROWS_DEV = 64
LANES = 128
PACK = LANES // RANK
JA = ("yl", "co")
IA_KA = ("ia", "ka")
IA_YL = ("ia", "yl")
IA_JA = ("ia", "yl", "co")
CO_KA = ("co", "ka")
YL_KA = ("yl", "ka")
IA_JA_KA = ("ia", "yl", "co", "ka")
BF16 = jnp.bfloat16
F32 = jnp.float32
VMEM = pl.BlockSpec(memory_space=pltpu.VMEM)
SMEM = pl.BlockSpec(memory_space=pltpu.SMEM)
HBM = pl.BlockSpec(memory_space=pltpu.HBM)


def iota(shape, dim):
    return lax.broadcasted_iota(jnp.int32, shape, dim)


def exchange(x, axes):
    return lax.all_to_all(x, axes, split_axis=0, concat_axis=0, tiled=True)


def to_everyone(x, axes):
    return exchange(jnp.broadcast_to(x, (lax.axis_size(axes), *x.shape)), axes)


def turn(ranks, turned, first=0):
    for g in range(ranks.shape[0] // LANES):
        turned[first + g] = ranks[g * LANES : (g + 1) * LANES, :].T


def fetch_rows(views, table, rows, start, count, high):
    for r in range(count):
        rows[pl.ds(r * high, high), :] = table[pl.ds(views[r][start], high), :]


def views_of(index, count):
    return [index.at[pl.ds(r, index.shape[0] - r)] for r in range(count)]


def scaled_body(cols, x, ranks, out, table, turned, picks, rows, scaled, index, values, done, ready):
    indices = pltpu.make_async_copy(cols, index, ready.at[0])
    values_in = pltpu.make_async_copy(x, values, ready.at[1])
    indices.start()
    values_in.start()
    turn(ranks, turned)
    groups = turned.shape[0]
    row, lane = iota((LANES, KR), 0), iota((LANES, KR), 1)
    for j in range(PACK):
        picks[j] = (((row >> 4) == j) & ((row & 15) == (lane >> 4))).astype(BF16)

    def pick(j, _):
        for g in range(groups):
            both = jnp.dot(turned[g], picks[j], preferred_element_type=F32)
            start = pl.multiple_of((g * PACK + j) * 2 * LANES, 2 * LANES)
            table[pl.ds(start, LANES, 2), :] = both[:, :LANES]
            table[pl.ds(start + 1, LANES, 2), :] = both[:, LANES:]
        return 0

    lax.fori_loop(0, PACK, pick, 0)
    indices.wait()
    values_in.wait()
    tiles = x.shape[1]
    count = tiles * LANES
    views = views_of(index, count)

    def sent(g):
        part = pl.ds(pl.multiple_of(g * count, count), count)
        return pltpu.make_async_copy(scaled.at[part], out.at[part], done.at[g])

    def group(g, _):
        fetch_rows(views, table, rows, g * count, count, 2)
        xs = values[g].astype(F32).T
        for j in range(tiles):
            by = xs[:, j : j + 1]
            left = rows[pl.ds(j * 2 * LANES, LANES, 2), :] * by
            right = rows[pl.ds(j * 2 * LANES + 1, LANES, 2), :] * by
            start = pl.multiple_of(g * count + j * LANES, LANES)
            scaled[pl.ds(start, LANES), :] = jnp.concatenate([left, right], axis=1).astype(BF16)
        sent(g).start()
        return 0

    lax.fori_loop(0, x.shape[0], group, 0)

    def wait(g, _):
        sent(g).wait()
        return 0

    lax.fori_loop(0, x.shape[0], wait, 0)


def partial_body(depths, scaled, target, ranks, ranks_other, out, table, turned, picks, rows, index, left, done):
    indices = pltpu.make_async_copy(depths, index, done.at[0])
    lefts = pltpu.make_async_copy(scaled, left, done.at[1])
    indices.start()
    lefts.start()
    turn(ranks, turned)
    turn(ranks_other, turned, turned.shape[0] // 2)
    groups = turned.shape[0]
    row, lane = iota((LANES, 2 * LANES), 0), iota((LANES, 2 * LANES), 1)
    for j in range(PACK // 2):
        picks[j] = (((row >> 4) == 2 * j + (lane >> 7)) & ((row & 15) == (lane & 15))).astype(BF16)

    def pick(j, _):
        for g in range(groups):
            two = jnp.dot(turned[g], picks[j], preferred_element_type=F32)
            start = pl.multiple_of((g * PACK + 2 * j) * LANES, 2 * LANES)
            table[pl.ds(start, LANES), :] = two[:, :LANES]
            table[pl.ds(start + LANES, LANES), :] = two[:, LANES:]
        return 0

    lax.fori_loop(0, PACK // 2, pick, 0)
    indices.wait()
    step = 8 * LANES
    views = views_of(index, step)

    def several_rows(g, _):
        start = pl.multiple_of(g * step, step)
        fetch_rows(views, table, rows.at[pl.ds(start, step)], start, step, 1)
        return 0

    lax.fori_loop(0, rows.shape[0] // step, several_rows, 0)
    lefts.wait()
    owners, slots, _ = target.shape
    count = slots * LANES
    together = 2

    def several(i, _):
        for k in range(together):
            o = i * together + k
            start = pl.multiple_of(o * count, LANES)
            right = rows[pl.ds(start, count), :].astype(BF16)
            kron = left[pl.ds(start, count), :] * jnp.concatenate([right, right], axis=1)
            owner_rows = target[o]
            hits = [(iota((ROWS_DEV, LANES), 0) == owner_rows[t : t + 1, :]).astype(BF16) for t in range(slots)]
            block = jnp.dot(jnp.concatenate(hits, axis=1), kron, preferred_element_type=F32)
            place = ((o >> 2) & 1) * (owners // 2) + (o >> 3) * 4 + (o & 3)
            out[place] = block.astype(BF16)
        return 0

    lax.fori_loop(0, owners // together, several, 0)


def added(copies):
    total = copies[0].astype(F32)
    for s in range(1, copies.shape[0]):
        total = total + copies[s].astype(F32)
    return total


def finish_body(arrived, proj, y, pieces, new_factor):
    total = added(arrived)
    y[...] = total
    gram = lax.dot_general(
        total, total, (((0,), (0,)), ((), ())), precision=lax.Precision.HIGHEST, preferred_element_type=F32
    )
    pieces[...] = gram.astype(BF16).reshape(pieces.shape)
    new_factor[...] = lax.dot_general(
        proj[...], total, (((1,), (1,)), ((), ())), precision=lax.Precision.HIGHEST, preferred_element_type=F32
    )


def cost(flops, nbytes):
    return pl.CostEstimate(flops=flops, transcendentals=0, bytes_accessed=nbytes)


def call(body, out_shape, in_specs, args, scratch=(), limit=16, flops=10**9, out_spec=VMEM):
    several = isinstance(out_shape, tuple)
    return pl.pallas_call(
        body,
        out_shape=out_shape,
        in_specs=in_specs,
        out_specs=(out_spec,) * len(out_shape) if several else out_spec,
        scratch_shapes=list(scratch),
        cost_estimate=cost(flops, 10**6),
        compiler_params=pltpu.CompilerParams(vmem_limit_bytes=limit * 2**20),
    )(*args)


def scaled_rows(cols, x, ranks):
    groups, tiles, _ = x.shape
    x = pltpu.with_memory_space_constraint(x, pltpu.HBM)
    out = pltpu.HBM((cols.shape[0], KR), BF16)
    scratch = [
        pltpu.VMEM((ranks.shape[0] * PACK * 2, LANES), F32),
        pltpu.VMEM((ranks.shape[0] // LANES, LANES, LANES), BF16),
        pltpu.VMEM((PACK, LANES, KR), BF16),
        pltpu.VMEM((tiles * LANES * 2, LANES), F32),
        pltpu.VMEM(out.shape, BF16),
        pltpu.SMEM(cols.shape, jnp.int32),
        pltpu.VMEM(x.shape, BF16),
        pltpu.SemaphoreType.DMA((groups,)),
        pltpu.SemaphoreType.DMA((2,)),
    ]
    return call(scaled_body, out, [HBM, HBM, VMEM], (cols, x, ranks), scratch, limit=24, out_spec=HBM)


def partial_blocks(depths, scaled, target, ranks, ranks_other):
    owners = target.shape[0]
    groups = 2 * ranks.shape[0] // LANES
    out = jax.ShapeDtypeStruct((owners, ROWS_DEV, KR), BF16)
    scratch = [
        pltpu.VMEM((groups * PACK * LANES, LANES), F32),
        pltpu.VMEM((groups, LANES, LANES), BF16),
        pltpu.VMEM((PACK // 2, LANES, 2 * LANES), BF16),
        pltpu.VMEM((depths.shape[0], LANES), F32),
        pltpu.SMEM(depths.shape, jnp.int32),
        pltpu.VMEM(scaled.shape, BF16),
        pltpu.SemaphoreType.DMA((2,)),
    ]
    scaled = pltpu.with_memory_space_constraint(scaled, pltpu.HBM)
    args = (depths, scaled, target, ranks, ranks_other)
    return call(partial_body, out, [HBM, HBM, VMEM, VMEM, VMEM], args, scratch, limit=32)


def finish(arrived, proj, parts):
    out = (
        jax.ShapeDtypeStruct((ROWS_DEV, KR), F32),
        jax.ShapeDtypeStruct((parts, KR // parts, KR), BF16),
        jax.ShapeDtypeStruct((RANK, ROWS_DEV), F32),
    )
    return call(finish_body, out, [VMEM, VMEM], (arrived, proj))


def added_copies(arrived, copies, scale=None):
    def body(arrived, out):
        total = added(arrived)
        total = (total if scale is None else total * scale).astype(BF16)
        for s in range(out.shape[0]):
            out[s] = total

    out = jax.ShapeDtypeStruct((copies, *arrived.shape[1:]), BF16)
    return call(body, out, [VMEM], (arrived,), flops=10**7)


def halves_added(arrived):
    def body(arrived, out):
        for s in range(out.shape[0]):
            out[s] = (arrived[0, s].astype(F32) + arrived[1, s].astype(F32)).astype(BF16)

    out = jax.ShapeDtypeStruct(arrived.shape[1:], BF16)
    return call(body, out, [VMEM], (arrived,), flops=10**7)


def update(tile_values, tile_rows, tile_cols, tile_depths, tile_live, factor_b, factor_c, proj):
    n_ia, n_yl, n_co, n_ka = (lax.axis_size(a) for a in IA_JA_KA)
    owners = n_yl * n_co * n_ka
    tiles, width = tile_values.shape
    slots = tiles // owners
    ranks_b = to_everyone(factor_b[:, 0, :], IA_KA).reshape(-1, LANES)
    for_c = jnp.broadcast_to(factor_c[:, 0, :], (n_ia * n_yl, RANK, LANES))
    ranks_c = exchange(for_c, IA_YL).reshape(-1, LANES)
    ranks_other = lax.ppermute(ranks_c, "co", [(0, 1), (1, 0)])
    block = tile_depths >> 7
    half = (block ^ lax.axis_index("co")) & 1
    depths = ((half * (n_ia * n_yl) + (block >> 1)) * LANES + (tile_depths & (LANES - 1))).reshape(-1)
    cols = (tile_cols * 2).reshape(-1)
    live = lax.iota(jnp.int32, slots)[None, :] < tile_live.reshape(owners, 1)
    target = jnp.where(live[:, :, None], tile_rows.reshape(owners, slots, width), ROWS_DEV)
    scaled = scaled_rows(cols, tile_values.reshape(tiles // PACK, PACK, width), ranks_b)
    blocks = partial_blocks(depths, scaled, target, ranks_c, ranks_other)
    halves = exchange(blocks, "co").reshape(n_co, owners // n_co, ROWS_DEV, KR)
    arrived = exchange(halves_added(halves), YL_KA)
    y, pieces, new_factor = finish(arrived, proj, n_co * n_ka)
    mine = added_copies(exchange(pieces, CO_KA), n_yl)
    mine = added_copies(exchange(mine, "yl"), n_ia)
    mine = added_copies(exchange(mine, "ia"), n_co * n_ka, 1.0 / (ROWS_DEV * owners * n_ia))
    gram = exchange(mine, CO_KA).reshape(KR, KR).astype(F32)
    return y, gram, new_factor


def solution(mesh):
    n_ka = mesh.shape["ka"]
    finer = Mesh(mesh.devices.reshape(-1, 4, 2, n_ka), IA_JA_KA)
    in_specs = (
        P(IA_JA_KA, None),
        P(IA_JA_KA, None),
        P(IA_JA_KA, None),
        P(IA_JA_KA, None),
        P(IA_JA_KA, None),
        P(None, JA, IA_KA),
        P(None, "ka", IA_JA),
        P(),
    )
    out_specs = (P(IA_JA_KA, None), P(), P(None, IA_JA_KA))
    return jax.shard_map(update, mesh=finer, in_specs=in_specs, out_specs=out_specs, check_vma=False)
```
